8 devices in a mesh: rep: 1 (over z), mp: 2 (over y), tok: 4 (over x, core).
Axes of the slice: x: 2, y: 2, z: 1, core: 2. Of those that a mesh axis runs over, the one named last changes fastest.
Arguments:
- hidden_in: bfloat16 [16384, 768], P(('rep', 'tok', 'mp'))
- seg_ids: int32 [16384], P(('rep', 'tok', 'mp'))
- expert_ids: int32 [16384, 2], P(('rep', 'tok', 'mp'))
- expert_gates: float32 [16384, 2], P(('rep', 'tok', 'mp'))
- w_query: bfloat16 [2, 768, 12, 64], P(None, 'tok', 'mp')
- w_key: bfloat16 [2, 768, 12, 64], P(None, 'tok', 'mp')
- w_value: bfloat16 [2, 768, 12, 64], P(None, 'tok', 'mp')
- w_out: bfloat16 [2, 12, 64, 768], P(None, 'mp', None, 'tok')
- w_gate: bfloat16 [2, 32, 768, 3072], P(None, None, 'tok', 'mp')
- w_up: bfloat16 [2, 32, 768, 3072], P(None, None, 'tok', 'mp')
- w_down: bfloat16 [2, 32, 3072, 768], P(None, None, 'mp', 'tok')
- gain_attn: bfloat16 [2, 768], replicated
- gain_mlp: bfloat16 [2, 768], replicated
Outputs:
- output: float32 [16384, 768], P(('rep', 'tok', 'mp'))
All inputs are finite; a program needn't handle non-finite values.
Results may differ from the reference program's by a relative error of at most 0.00981009.
Values are sent between devices in bfloat16 or wider.
A program may use at most 1 GiB of HBM per device.

```python
import jax
import jax.numpy as jnp
from jax import lax

TOKENS = 16384
SHARDS = 4
HIDDEN = 768
FFN_WIDTH = 3072
Q_HEADS = 12
KV_HEADS = 12
HEAD_DIM = 64
EXPERTS = 32
NUM_LAYERS = 2
REQ_CUTS = 3

SHARD_LEN = TOKENS // SHARDS
QUERY_BLOCK = min(SHARD_LEN, 256)
EPS = 1e-5
ROPE_BASE = 10000.0


def normal_weight(key, shape, scale):
    return (jax.random.normal(key, shape, jnp.float32) * scale).astype(jnp.bfloat16)


def setup_inputs(seed: int = 0, part: int = 0) -> dict:
    base_key = jax.random.key(seed)
    part_keys = jax.random.split(jax.random.fold_in(base_key, part), 5)
    weight_keys = jax.random.split(jax.random.key(seed + 1), 9)
    hidden_in = jax.random.normal(part_keys[0], (TOKENS, HIDDEN), jnp.float32).astype(jnp.bfloat16)
    cut_points = jax.random.randint(part_keys[1], (SHARDS, 1, REQ_CUTS), 1, SHARD_LEN)
    token_pos = jnp.arange(SHARD_LEN, dtype=jnp.int32)[None, :, None]
    req_index = jnp.sum((token_pos >= cut_points).astype(jnp.int32), axis=-1)
    shard_base = jnp.arange(SHARDS, dtype=jnp.int32)[:, None] * (REQ_CUTS + 1)
    seg_ids = (shard_base + req_index).reshape(TOKENS).astype(jnp.int32)
    first_pick = jax.random.permutation(part_keys[2], jnp.arange(TOKENS, dtype=jnp.int32) % EXPERTS)
    pick_shift = jax.random.randint(part_keys[3], (TOKENS,), 1, EXPERTS)
    second_pick = (first_pick + pick_shift) % EXPERTS
    expert_ids = jnp.stack([first_pick, second_pick], axis=1).astype(jnp.int32)
    top_share = jax.random.uniform(part_keys[4], (TOKENS,), jnp.float32, 0.3, 0.9)
    expert_gates = jnp.stack([top_share, 1.0 - top_share], axis=1)
    qk_scale = 1.4 * HIDDEN ** -0.5
    return {
        'hidden_in': hidden_in,
        'seg_ids': seg_ids,
        'expert_ids': expert_ids,
        'expert_gates': expert_gates,
        'w_query': normal_weight(weight_keys[0], (NUM_LAYERS, HIDDEN, Q_HEADS, HEAD_DIM), qk_scale),
        'w_key': normal_weight(weight_keys[1], (NUM_LAYERS, HIDDEN, KV_HEADS, HEAD_DIM), qk_scale),
        'w_value': normal_weight(weight_keys[2], (NUM_LAYERS, HIDDEN, KV_HEADS, HEAD_DIM), HIDDEN ** -0.5),
        'w_out': normal_weight(weight_keys[3], (NUM_LAYERS, Q_HEADS, HEAD_DIM, HIDDEN), 2.0 * (Q_HEADS * HEAD_DIM) ** -0.5),
        'w_gate': normal_weight(weight_keys[4], (NUM_LAYERS, EXPERTS, HIDDEN, FFN_WIDTH), HIDDEN ** -0.5),
        'w_up': normal_weight(weight_keys[5], (NUM_LAYERS, EXPERTS, HIDDEN, FFN_WIDTH), HIDDEN ** -0.5),
        'w_down': normal_weight(weight_keys[6], (NUM_LAYERS, EXPERTS, FFN_WIDTH, HIDDEN), FFN_WIDTH ** -0.5),
        'gain_attn': jax.random.uniform(weight_keys[7], (NUM_LAYERS, HIDDEN), jnp.float32, 0.5, 1.5).astype(jnp.bfloat16),
        'gain_mlp': jax.random.uniform(weight_keys[8], (NUM_LAYERS, HIDDEN), jnp.float32, 0.5, 1.5).astype(jnp.bfloat16),
    }


def rms_norm(residual, gain):
    inv_rms = lax.rsqrt(jnp.mean(residual * residual, axis=-1, keepdims=True) + EPS)
    return (residual * inv_rms * gain.astype(jnp.float32)).astype(jnp.bfloat16)


def request_positions(seg_shard):
    token_index = jnp.arange(SHARD_LEN, dtype=jnp.int32)
    is_start = jnp.concatenate([jnp.ones((1,), dtype=jnp.bool_), seg_shard[1:] != seg_shard[:-1]])
    start_index = lax.cummax(jnp.where(is_start, token_index, 0), axis=0)
    return token_index - start_index


def apply_rope(vectors, positions):
    half_dim = HEAD_DIM // 2
    inv_freq = jnp.power(ROPE_BASE, -jnp.arange(half_dim, dtype=jnp.float32) * 2.0 / HEAD_DIM)
    angles = positions.astype(jnp.float32)[:, None, None] * inv_freq
    cosines = jnp.cos(angles)
    sines = jnp.sin(angles)
    first_half = vectors[..., :half_dim]
    second_half = vectors[..., half_dim:]
    return jnp.concatenate([first_half * cosines - second_half * sines, second_half * cosines + first_half * sines], axis=-1)


def shard_attention(h_shard, seg_shard, q_weight, k_weight, v_weight):
    groups = Q_HEADS // KV_HEADS
    positions = request_positions(seg_shard)
    q_proj = jnp.dot(h_shard, q_weight.reshape(HIDDEN, Q_HEADS * HEAD_DIM), preferred_element_type=jnp.float32)
    k_proj = jnp.dot(h_shard, k_weight.reshape(HIDDEN, KV_HEADS * HEAD_DIM), preferred_element_type=jnp.float32)
    v_proj = jnp.dot(h_shard, v_weight.reshape(HIDDEN, KV_HEADS * HEAD_DIM), preferred_element_type=jnp.float32)
    q_rot = apply_rope(q_proj.reshape(SHARD_LEN, Q_HEADS, HEAD_DIM), positions).astype(jnp.bfloat16)
    k_rot = apply_rope(k_proj.reshape(SHARD_LEN, KV_HEADS, HEAD_DIM), positions).astype(jnp.bfloat16)
    keys32 = k_rot.astype(jnp.float32)
    values32 = v_proj.astype(jnp.bfloat16).astype(jnp.float32).reshape(SHARD_LEN, KV_HEADS, HEAD_DIM)
    token_index = jnp.arange(SHARD_LEN, dtype=jnp.int32)
    num_blocks = SHARD_LEN // QUERY_BLOCK
    q_blocks = q_rot.reshape(num_blocks, QUERY_BLOCK, KV_HEADS, groups, HEAD_DIM)

    def one_block(block_in):
        q_block, seg_block, index_block = block_in
        scores = jnp.einsum('bhgd,shd->hgbs', q_block.astype(jnp.float32), keys32) * HEAD_DIM ** -0.5
        allowed = (seg_block[:, None] == seg_shard[None, :]) & (token_index[None, :] <= index_block[:, None])
        attn_prob = jax.nn.softmax(jnp.where(allowed, scores, -1e30), axis=-1)
        attn_prob = attn_prob.astype(jnp.bfloat16).astype(jnp.float32)
        attn_out = jnp.einsum('hgbs,shd->bhgd', attn_prob, values32)
        return attn_out.astype(jnp.bfloat16).reshape(QUERY_BLOCK, Q_HEADS * HEAD_DIM)

    block_outs = lax.map(one_block, (q_blocks, seg_shard.reshape(num_blocks, QUERY_BLOCK), token_index.reshape(num_blocks, QUERY_BLOCK)))
    return block_outs.reshape(SHARD_LEN, Q_HEADS * HEAD_DIM)


def expert_mix(normed, expert_ids, expert_gates, gate_weight, up_weight, down_weight):
    def one_expert(mix_sum, expert_in):
        gate_mat, up_mat, down_mat, expert_num = expert_in
        gate_pre = jnp.dot(normed, gate_mat, preferred_element_type=jnp.float32)
        up_pre = jnp.dot(normed, up_mat, preferred_element_type=jnp.float32)
        hidden_act = (jax.nn.silu(gate_pre) * up_pre).astype(jnp.bfloat16)
        down_out = jnp.dot(hidden_act, down_mat, preferred_element_type=jnp.float32)
        route_weight = jnp.sum(jnp.where(expert_ids == expert_num, expert_gates, 0.0), axis=1)
        return mix_sum + route_weight[:, None] * down_out, None

    start_sum = jnp.zeros((normed.shape[0], HIDDEN), jnp.float32)
    mix_sum, _ = lax.scan(one_expert, start_sum, (gate_weight, up_weight, down_weight, jnp.arange(EXPERTS, dtype=jnp.int32)))
    return mix_sum


def reference(hidden_in, seg_ids, expert_ids, expert_gates, w_query, w_key, w_value, w_out, w_gate, w_up, w_down, gain_attn, gain_mlp):
    seg_shards = seg_ids.reshape(SHARDS, SHARD_LEN)

    def one_layer(residual, layer_in):
        q_weight, k_weight, v_weight, o_weight, gate_weight, up_weight, down_weight, attn_gain, mlp_gain = layer_in
        normed = rms_norm(residual, attn_gain).reshape(SHARDS, SHARD_LEN, HIDDEN)
        attn_out = lax.map(lambda shard_in: shard_attention(shard_in[0], shard_in[1], q_weight, k_weight, v_weight), (normed, seg_shards))
        attn_out = attn_out.reshape(TOKENS, Q_HEADS * HEAD_DIM)
        residual = residual + jnp.dot(attn_out, o_weight.reshape(Q_HEADS * HEAD_DIM, HIDDEN), preferred_element_type=jnp.float32)
        normed = rms_norm(residual, mlp_gain)
        residual = residual + expert_mix(normed, expert_ids, expert_gates, gate_weight, up_weight, down_weight)
        return residual, None

    final, _ = lax.scan(one_layer, hidden_in.astype(jnp.float32), (w_query, w_key, w_value, w_out, w_gate, w_up, w_down, gain_attn, gain_mlp))
    return final
```

```python
import functools

import jax
import jax.numpy as jnp
from jax import lax
from jax.experimental import pallas as pl
from jax.experimental.pallas import tpu as pltpu
from jax.sharding import PartitionSpec as P

EPS = 1e-5
ROPE_BASE = 10000.0
NEG = -1e30
VMEM_LIMIT = 66_000_000
ROW_TILE = 288
CHUNKS = 2


def rms_norm(residual, gain):
    inv_rms = lax.rsqrt(jnp.mean(residual * residual, axis=-1, keepdims=True) + EPS)
    return (residual * inv_rms * gain.astype(jnp.float32)).astype(jnp.bfloat16)


def request_starts(seg_row):
    token_index = jnp.arange(seg_row.shape[0], dtype=jnp.int32)
    is_start = jnp.concatenate([jnp.ones((1,), dtype=jnp.bool_), seg_row[1:] != seg_row[:-1]])
    return lax.cummax(jnp.where(is_start, token_index, 0), axis=0)


def qkv_kernel(x_ref, w_ref, cos_ref, sin_ref, q_ref, k_ref, v_ref):
    width = q_ref.shape[1]
    reps = width // cos_ref.shape[1]
    cosines = jnp.concatenate([cos_ref[...]] * reps, axis=1)
    sines = jnp.concatenate([sin_ref[...]] * reps, axis=1)
    proj = jnp.dot(x_ref[...], w_ref[...], preferred_element_type=jnp.float32)
    q_ref[...] = ((proj[:, :width] * cosines + proj[:, width:2 * width] * sines) * 0.125).astype(jnp.bfloat16)
    k_ref[...] = (proj[:, 2 * width:3 * width] * cosines + proj[:, 3 * width:4 * width] * sines).astype(jnp.bfloat16)
    v_ref[...] = proj[:, 4 * width:].astype(jnp.bfloat16)


def project_qkv(normed, weight, cosines, sines):
    rows, hidden = normed.shape
    width = weight.shape[1] // 5
    block = 512
    row_block = pl.BlockSpec((block, width), lambda i: (i, 0))
    table = pl.BlockSpec((block, cosines.shape[1]), lambda i: (i, 0))
    return pl.pallas_call(
        qkv_kernel,
        grid=(rows // block,),
        in_specs=[pl.BlockSpec((block, hidden), lambda i: (i, 0)), pl.BlockSpec(weight.shape, lambda i: (0, 0)), table, table],
        out_specs=[row_block] * 3,
        out_shape=[jax.ShapeDtypeStruct((rows, width), jnp.bfloat16)] * 3,
        compiler_params=pltpu.CompilerParams(vmem_limit_bytes=VMEM_LIMIT),
        cost_estimate=pl.CostEstimate(flops=2 * rows * hidden * weight.shape[1], bytes_accessed=16 * 1024 * 1024, transcendentals=0),
        name="qkv",
    )(normed, weight, cosines, sines)


def attention_kernel(first_ref, q_ref, k_ref, v_ref, start_ref, o_ref):
    block = q_ref.shape[0]
    i = pl.program_id(1)
    q = q_ref[...]
    lane = lax.broadcasted_iota(jnp.int32, q.shape, 1)
    q_heads = [jnp.where(lane < 64, q, jnp.zeros_like(q)), jnp.where(lane < 64, jnp.zeros_like(q), q)]
    start = start_ref[...]
    row = i * block + lax.broadcasted_iota(jnp.int32, (block, block), 0)
    col = lax.broadcasted_iota(jnp.int32, (block, block), 1)

    def step(j, carry):
        keys = k_ref[pl.ds(pl.multiple_of(j * block, block), block), :]
        values = v_ref[pl.ds(pl.multiple_of(j * block, block), block), :]
        at = col + j * block
        allowed = (at >= start) & (at <= row)
        out = []
        for head in range(2):
            top, total, acc = carry[head]
            scores = lax.dot_general(q_heads[head], keys, (((1,), (1,)), ((), ())), preferred_element_type=jnp.float32)
            scores = jnp.where(allowed, scores, NEG)
            new_top = jnp.maximum(top, jnp.max(scores, axis=1, keepdims=True))
            prob = jnp.exp(scores - new_top)
            decay = jnp.exp(top - new_top)
            total = total * decay + jnp.sum(prob, axis=1, keepdims=True)
            acc = acc * decay + jnp.dot(prob.astype(jnp.bfloat16), values, preferred_element_type=jnp.float32)
            out.append((new_top, total, acc))
        return tuple(out)

    zero = (jnp.full((block, 1), NEG, jnp.float32), jnp.zeros((block, 1), jnp.float32), jnp.zeros(q.shape, jnp.float32))
    (_, total_a, acc_a), (_, total_b, acc_b) = lax.fori_loop(first_ref[i], i + 1, step, (zero, zero))
    o_ref[...] = jnp.where(lane < 64, acc_a / total_a, acc_b / total_b).astype(jnp.bfloat16)


def attention(q, k, v, starts):
    rows, width = q.shape
    block = 512
    first = starts[::block] // block
    grid_spec = pltpu.PrefetchScalarGridSpec(
        num_scalar_prefetch=1,
        grid=(width // 128, rows // block),
        in_specs=[
            pl.BlockSpec((block, 128), lambda p, i, f: (i, p)),
            pl.BlockSpec((rows, 128), lambda p, i, f: (0, p)),
            pl.BlockSpec((rows, 128), lambda p, i, f: (0, p)),
            pl.BlockSpec((block, 1), lambda p, i, f: (i, 0)),
        ],
        out_specs=pl.BlockSpec((block, 128), lambda p, i, f: (i, p)),
    )
    return pl.pallas_call(
        attention_kernel,
        grid_spec=grid_spec,
        out_shape=jax.ShapeDtypeStruct((rows, width), jnp.bfloat16),
        compiler_params=pltpu.CompilerParams(vmem_limit_bytes=VMEM_LIMIT),
        cost_estimate=pl.CostEstimate(flops=8 * rows * rows * width, bytes_accessed=16 * 1024 * 1024, transcendentals=rows * rows * 3),
        name="attention",
    )(first, q, k, v, starts[:, None])


def moe_kernel(tile_expert, tile_start, tile_count, place, token_ref, gate_ref, h_ref, g0, g1, g2, g3, u0, u1, u2, u3, d0, d1, d2, d3, out_ref, x_scr, y_scr, wg, wu, wd):
    i = pl.program_id(0)
    depth = g0.shape[1]

    @pl.when(i == 0)
    def _():
        out_ref[...] = jnp.zeros_like(out_ref)
        x_scr[...] = jnp.zeros_like(x_scr)

    @pl.when(i < place[1])
    def _():
        start, count = tile_start[i], tile_count[i]

        @pl.when((i == 0) | (tile_expert[i] != tile_expert[jnp.maximum(i - 1, 0)]))
        def _():
            for home in range(4):
                @pl.when(place[0] == home)
                def _():
                    for j, (g, u, d) in enumerate(((g0, u0, d0), (g1, u1, d1), (g2, u2, d2), (g3, u3, d3))):
                        at = (home ^ j) * depth
                        wg[at:at + depth, :] = g[0]
                        wu[at:at + depth, :] = u[0]
                        wd[:, at:at + depth] = d[0]

        def fetch(b, _):
            base = pl.multiple_of(b * 8, 8)
            rows = [h_ref[pl.ds(token_ref[start + base + r], 1), :] for r in range(8)]
            x_scr[pl.ds(base, 8), :] = jnp.concatenate(rows, axis=0)
            return 0

        lax.fori_loop(0, lax.div(count + 7, 8), fetch, 0)
        x = x_scr[...].astype(jnp.bfloat16)
        gate_pre = jnp.dot(x, wg[...], preferred_element_type=jnp.float32)
        up_pre = jnp.dot(x, wu[...], preferred_element_type=jnp.float32)
        act = (gate_pre * jax.nn.sigmoid(gate_pre) * up_pre).astype(jnp.bfloat16)
        y_scr[...] = jnp.dot(act, wd[...], preferred_element_type=jnp.float32)

        def add_eight(b, _):
            base = pl.multiple_of(b * 8, 8)
            part = y_scr[pl.ds(base, 8), :]
            tokens = [token_ref[start + base + r] for r in range(8)]
            sums = [out_ref[pl.ds(tokens[r], 1), :] + part[r:r + 1, :] * gate_ref[start + base + r] for r in range(8)]
            for r in range(8):
                out_ref[pl.ds(tokens[r], 1), :] = sums[r]
            return 0

        def add_one(r, _):
            token = token_ref[start + r]
            out_ref[pl.ds(token, 1), :] = out_ref[pl.ds(token, 1), :] + y_scr[pl.ds(r, 1), :] * gate_ref[start + r]
            return 0

        full = lax.div(count, 8)
        lax.fori_loop(0, full, add_eight, 0)
        lax.fori_loop(full * 8, count, add_one, 0)


def run_experts(h_rows, tables, place, tokens, gates, gate_parts, up_parts, down_parts):
    tile_expert, tile_start, tile_count, num_tiles = tables
    place = jnp.stack([place, num_tiles])
    rows, hidden = h_rows.shape
    _, depth, width = gate_parts[0].shape
    whole = lambda i, *_: (0, 0)
    pick = lambda i, te, *_: (te[i], 0, 0)
    grid_spec = pltpu.PrefetchScalarGridSpec(
        num_scalar_prefetch=6,
        grid=(tile_expert.shape[0],),
        in_specs=[pl.BlockSpec((rows, hidden), whole, pipeline_mode=pl.Buffered(1))]
        + [pl.BlockSpec((1, depth, width), pick)] * 8
        + [pl.BlockSpec((1, width, depth), pick)] * 4,
        out_specs=pl.BlockSpec((rows, hidden), whole, pipeline_mode=pl.Buffered(1)),
        scratch_shapes=[
            pltpu.VMEM((ROW_TILE, hidden), jnp.float32),
            pltpu.VMEM((ROW_TILE, hidden), jnp.float32),
            pltpu.VMEM((hidden, width), jnp.bfloat16),
            pltpu.VMEM((hidden, width), jnp.bfloat16),
            pltpu.VMEM((width, hidden), jnp.bfloat16),
        ],
    )
    experts = gate_parts[0].shape[0]
    return pl.pallas_call(
        moe_kernel,
        grid_spec=grid_spec,
        out_shape=jax.ShapeDtypeStruct((rows, hidden), jnp.float32),
        compiler_params=pltpu.CompilerParams(vmem_limit_bytes=VMEM_LIMIT),
        cost_estimate=pl.CostEstimate(flops=12 * 256 * experts * hidden * width, bytes_accessed=80 * 1024 * 1024, transcendentals=0),
        name="experts",
    )(tile_expert, tile_start, tile_count, place, tokens, gates, h_rows, *gate_parts, *up_parts, *down_parts)


def tile_tables(sizes, first_expert, experts, max_pairs):
    order = jnp.arange(sizes.shape[0], dtype=jnp.int32)
    offsets = jnp.sum(jnp.where(order[None, :] < order[:, None], sizes[None, :], 0), axis=1)
    count = lax.dynamic_slice_in_dim(sizes, first_expert, experts)
    offset = lax.dynamic_slice_in_dim(offsets, first_expert, experts)
    tiles = (count + ROW_TILE - 1) // ROW_TILE
    local = jnp.arange(experts, dtype=jnp.int32)
    first_tile = jnp.sum(jnp.where(local[None, :] < local[:, None], tiles[None, :], 0), axis=1)
    num_tiles = jnp.sum(tiles)
    last = jnp.max(jnp.where(tiles > 0, local, 0))
    max_tiles = (max_pairs - experts) // ROW_TILE + experts
    tile = jnp.arange(max_tiles, dtype=jnp.int32)
    mine = (tile[:, None] >= first_tile[None, :]) & (tile[:, None] < (first_tile + tiles)[None, :])
    pick = lambda values: jnp.sum(jnp.where(mine, values, 0), axis=1).astype(jnp.int32)
    done = (tile[:, None] - first_tile[None, :]) * ROW_TILE
    return jnp.where(tile < num_tiles, pick(local[None, :]), last), pick(offset[None, :] + done), pick(jnp.minimum(count[None, :] - done, ROW_TILE)), num_tiles.astype(jnp.int32)


def solution(mesh):
    token_spec = P(('rep', 'tok', 'mp'))
    row_spec = P(('rep', 'tok', 'mp'), None)
    head_weight = P(None, 'tok', 'mp', None)
    in_specs = (row_spec, token_spec, row_spec, row_spec, head_weight, head_weight, head_weight, P(None, 'mp', None, 'tok'), P(None, None, 'tok', 'mp'), P(None, None, 'tok', 'mp'), P(None, None, 'mp', 'tok'), P(None, None), P(None, None))

    def swap_mp(value):
        return lax.ppermute(value, 'mp', [(0, 1), (1, 0)])

    def swap_chip(value):
        return lax.ppermute(value, 'tok', [(i, i ^ 2) for i in range(4)])

    def swap_core(value):
        return lax.ppermute(value, 'tok', [(i, i ^ 1) for i in range(4)])

    def swap_diagonal(value):
        return lax.ppermute(value, ('mp', 'tok'), [(i, i ^ 6) for i in range(8)])

    def device_step(hidden_in, seg_ids, expert_ids, expert_gates, w_query, w_key, w_value, w_out, w_gate, w_up, w_down, gain_attn, gain_mlp):
        num_layers, depth, q_local, head_dim = w_query.shape
        num_experts = w_gate.shape[1]
        rows, hidden = hidden_in.shape
        half_experts = num_experts // 2
        chunk = half_experts // CHUNKS
        m = lax.axis_index('mp')
        t = lax.axis_index('tok')
        chip = t // 2
        place = t.astype(jnp.int32)

        def join(mine, other, axis=0):
            first = jnp.where(m == 0, mine, other)
            second = jnp.where(m == 0, other, mine)
            return jnp.concatenate([first, second], axis=axis)

        def gather_mp(value):
            return join(value, swap_mp(value))

        qkv_local = jnp.concatenate([w.reshape(num_layers, depth, q_local * head_dim) for w in (w_query, w_key, w_value)], axis=2)
        qkv_all = lax.all_gather(qkv_local, 'tok', axis=1, tiled=True)
        out_all = lax.all_gather(w_out.reshape(num_layers, q_local * head_dim, depth), ('mp', 'tok'), axis=0)
        out_all = out_all.reshape(2, 4, num_layers, q_local * head_dim, depth).transpose(2, 0, 3, 1, 4).reshape(num_layers, 2 * q_local * head_dim, hidden)

        def rotated(weight):
            parts = weight.reshape(hidden, q_local, 2, head_dim // 2)
            return jnp.concatenate([-parts[:, :, 1:], parts[:, :, :1]], axis=2).reshape(hidden, q_local * head_dim)

        seg_full = gather_mp(seg_ids)
        starts = request_starts(seg_full)
        seq_len = seg_full.shape[0]
        positions = jnp.arange(seq_len, dtype=jnp.int32) - starts
        inv_freq = jnp.power(ROPE_BASE, -jnp.arange(head_dim // 2, dtype=jnp.float32) * 2.0 / head_dim)
        angles = positions.astype(jnp.float32)[:, None] * inv_freq
        cosines = jnp.tile(jnp.cos(angles), (1, 4))
        sines = jnp.tile(jnp.sin(angles), (1, 4))

        flat_ids = gather_mp(expert_ids).reshape(2 * seq_len)
        flat_gates = gather_mp(expert_gates).reshape(2 * seq_len)
        pair_token = jnp.arange(2 * seq_len, dtype=jnp.int32) // 2
        _, tokens_own, gates_own = lax.sort((flat_ids, pair_token, flat_gates), num_keys=1)
        sizes_own = jnp.sum((flat_ids[:, None] == jnp.arange(num_experts, dtype=jnp.int32)[None, :]).astype(jnp.int32), axis=0)
        pad = jnp.zeros((8,), jnp.int32)
        ints_own = jnp.concatenate([sizes_own, tokens_own, pad])
        floats_own = jnp.concatenate([gates_own, pad.astype(jnp.float32)])
        ints_far = swap_chip(ints_own)
        floats_far = swap_chip(floats_own)
        routing = []
        for ints, floats in ((ints_far, floats_far), (ints_own, floats_own)):
            tables = [tile_tables(ints[:num_experts], chip * half_experts + c * chunk, chunk, 2 * seq_len) for c in range(CHUNKS)]
            routing.append((tables, ints[num_experts:], floats))

        def exchange(weight, layer, c):
            near = lax.dynamic_slice_in_dim(weight[layer], chip * half_experts + c * chunk, chunk, 0)
            far = lax.dynamic_slice_in_dim(weight[layer], (1 - chip) * half_experts + c * chunk, chunk, 0)
            return near, far

        def spread(near, far):
            crossed = swap_chip(far)
            return near, swap_core(near), crossed, swap_core(crossed)

        residual = hidden_in.astype(jnp.float32)
        for layer in range(num_layers):
            q_w, k_w, v_w = jnp.split(qkv_all[layer], 3, axis=1)
            weight = jnp.concatenate([q_w, rotated(q_w), k_w, rotated(k_w), v_w], axis=1)
            normed = gather_mp(rms_norm(residual, gain_attn[layer]))
            q, k, v = project_qkv(normed, weight, cosines, sines)
            attn = attention(q, k, v, starts)
            keep = lax.dynamic_slice_in_dim(attn, m * rows, rows, 0)
            send = lax.dynamic_slice_in_dim(attn, (1 - m) * rows, rows, 0)
            attn_full = join(keep, swap_mp(send), axis=1)
            residual = residual + jnp.dot(attn_full, out_all[layer], preferred_element_type=jnp.float32)
            normed = rms_norm(residual, gain_mlp[layer])
            far_half = swap_chip(normed)
            h_own = gather_mp(normed).astype(jnp.float32)
            h_far = gather_mp(far_half).astype(jnp.float32)
            parts = [None, None]
            for c in range(CHUNKS):
                gate_parts, up_parts, down_parts = [spread(*exchange(w, layer, c)) for w in (w_gate, w_up, w_down)]
                for s, h_rows in enumerate((h_far, h_own)):
                    tables, tokens, gates = routing[s]
                    got = run_experts(h_rows, tables[c], place, tokens, gates, gate_parts, up_parts, down_parts)
                    parts[s] = got if parts[s] is None else parts[s] + got
            far_sum, own_sum = parts
            pick = lambda value, which: lax.dynamic_slice_in_dim(value, which * rows, rows, 0)
            from_chip = swap_chip(pick(far_sum, m))
            from_diagonal = swap_diagonal(pick(far_sum, 1 - m))
            from_mp = swap_mp(pick(own_sum, 1 - m))
            residual = residual + pick(own_sum, m) + from_mp + from_chip + from_diagonal
        return residual

    return jax.shard_map(device_step, mesh=mesh, in_specs=in_specs, out_specs=row_spec, check_vma=False)
```

```python
import jax
import jax.numpy as jnp
from jax import lax
from jax.experimental import pallas as pl
from jax.experimental.pallas import tpu as pltpu
from jax.sharding import PartitionSpec as P


EPS = 1e-5
ROPE_BASE = 10000.0
NEG = -1e30
VMEM_LIMIT = 66_000_000
ROW_TILE = 288
CHUNKS = 2


def rms_norm(residual, gain):
    inv_rms = lax.rsqrt(jnp.mean(residual * residual, axis=-1, keepdims=True) + EPS)
    return (residual * inv_rms * gain.astype(jnp.float32)).astype(jnp.bfloat16)


def request_starts(seg_row):
    token_index = jnp.arange(seg_row.shape[0], dtype=jnp.int32)
    is_start = jnp.concatenate([jnp.ones((1,), dtype=jnp.bool_), seg_row[1:] != seg_row[:-1]])
    return lax.cummax(jnp.where(is_start, token_index, 0), axis=0)


def qkv_kernel(x_ref, w_ref, cos_ref, sin_ref, q_ref, k_ref, v_ref):
    width = q_ref.shape[1]
    reps = width // cos_ref.shape[1]
    cosines = jnp.concatenate([cos_ref[...]] * reps, axis=1)
    sines = jnp.concatenate([sin_ref[...]] * reps, axis=1)
    proj = jnp.dot(x_ref[...], w_ref[...], preferred_element_type=jnp.float32)
    q_ref[...] = ((proj[:, :width] * cosines + proj[:, width:2 * width] * sines) * 0.125).astype(jnp.bfloat16)
    k_ref[...] = (proj[:, 2 * width:3 * width] * cosines + proj[:, 3 * width:4 * width] * sines).astype(jnp.bfloat16)
    v_ref[...] = proj[:, 4 * width:].astype(jnp.bfloat16)


def project_qkv(normed, weight, cosines, sines):
    rows, hidden = normed.shape
    width = weight.shape[1] // 5
    block = 512
    row_block = pl.BlockSpec((block, width), lambda i: (i, 0))
    table = pl.BlockSpec((block, cosines.shape[1]), lambda i: (i, 0))
    return pl.pallas_call(
        qkv_kernel,
        grid=(rows // block,),
        in_specs=[pl.BlockSpec((block, hidden), lambda i: (i, 0)), pl.BlockSpec(weight.shape, lambda i: (0, 0)), table, table],
        out_specs=[row_block] * 3,
        out_shape=[jax.ShapeDtypeStruct((rows, width), jnp.bfloat16)] * 3,
        compiler_params=pltpu.CompilerParams(vmem_limit_bytes=VMEM_LIMIT),
        name="qkv",
    )(normed, weight, cosines, sines)


def attention_kernel(first_ref, q_ref, k_ref, v_ref, start_ref, o_ref):
    block = q_ref.shape[0]
    i = pl.program_id(1)
    q = q_ref[...]
    lane = lax.broadcasted_iota(jnp.int32, q.shape, 1)
    q_heads = [jnp.where(lane < 64, q, jnp.zeros_like(q)), jnp.where(lane < 64, jnp.zeros_like(q), q)]
    start = start_ref[...]
    row = i * block + lax.broadcasted_iota(jnp.int32, (block, block), 0)
    col = lax.broadcasted_iota(jnp.int32, (block, block), 1)

    def step(j, carry):
        keys = k_ref[pl.ds(pl.multiple_of(j * block, block), block), :]
        values = v_ref[pl.ds(pl.multiple_of(j * block, block), block), :]
        at = col + j * block
        allowed = (at >= start) & (at <= row)
        out = []
        for head in range(2):
            top, total, acc = carry[head]
            scores = lax.dot_general(q_heads[head], keys, (((1,), (1,)), ((), ())), preferred_element_type=jnp.float32)
            scores = jnp.where(allowed, scores, NEG)
            new_top = jnp.maximum(top, jnp.max(scores, axis=1, keepdims=True))
            prob = jnp.exp(scores - new_top)
            decay = jnp.exp(top - new_top)
            total = total * decay + jnp.sum(prob, axis=1, keepdims=True)
            acc = acc * decay + jnp.dot(prob.astype(jnp.bfloat16), values, preferred_element_type=jnp.float32)
            out.append((new_top, total, acc))
        return tuple(out)

    zero = (jnp.full((block, 1), NEG, jnp.float32), jnp.zeros((block, 1), jnp.float32), jnp.zeros(q.shape, jnp.float32))
    (_, total_a, acc_a), (_, total_b, acc_b) = lax.fori_loop(first_ref[i], i + 1, step, (zero, zero))
    o_ref[...] = jnp.where(lane < 64, acc_a / total_a, acc_b / total_b).astype(jnp.bfloat16)


def attention(q, k, v, starts):
    rows, width = q.shape
    block = 512
    first = starts[::block] // block
    grid_spec = pltpu.PrefetchScalarGridSpec(
        num_scalar_prefetch=1,
        grid=(width // 128, rows // block),
        in_specs=[
            pl.BlockSpec((block, 128), lambda p, i, f: (i, p)),
            pl.BlockSpec((rows, 128), lambda p, i, f: (0, p)),
            pl.BlockSpec((rows, 128), lambda p, i, f: (0, p)),
            pl.BlockSpec((block, 1), lambda p, i, f: (i, 0)),
        ],
        out_specs=pl.BlockSpec((block, 128), lambda p, i, f: (i, p)),
    )
    return pl.pallas_call(
        attention_kernel,
        grid_spec=grid_spec,
        out_shape=jax.ShapeDtypeStruct((rows, width), jnp.bfloat16),
        compiler_params=pltpu.CompilerParams(vmem_limit_bytes=VMEM_LIMIT),
        name="attention",
    )(first, q, k, v, starts[:, None])


def moe_kernel(tile_expert, tile_start, tile_count, place, token_ref, gate_ref, h_ref, g0, g1, g2, g3, u0, u1, u2, u3, d0, d1, d2, d3, out_ref, x_scr, y_scr, wg, wu, wd):
    i = pl.program_id(0)
    depth = g0.shape[1]

    @pl.when(i == 0)
    def _():
        out_ref[...] = jnp.zeros_like(out_ref)
        x_scr[...] = jnp.zeros_like(x_scr)

    @pl.when(i < place[1])
    def _():
        start, count = tile_start[i], tile_count[i]

        @pl.when((i == 0) | (tile_expert[i] != tile_expert[jnp.maximum(i - 1, 0)]))
        def _():
            for j, (g, u, d) in enumerate(((g0, u0, d0), (g1, u1, d1), (g2, u2, d2), (g3, u3, d3))):
                at = pl.multiple_of((place[0] ^ j) * depth, depth)
                wg[pl.ds(at, depth), :] = g[0]
                wu[pl.ds(at, depth), :] = u[0]
                wd[pl.ds(at, depth), :] = d[0]

        def fetch(b, _):
            base = pl.multiple_of(b * 8, 8)
            rows = [h_ref[pl.ds(token_ref[start + base + r], 1), :] for r in range(8)]
            x_scr[pl.ds(base, 8), :] = jnp.concatenate(rows, axis=0)
            return 0

        lax.fori_loop(0, lax.div(count + 7, 8), fetch, 0)
        x = x_scr[...].astype(jnp.bfloat16)
        gate_pre = jnp.dot(x, wg[...], preferred_element_type=jnp.float32)
        up_pre = jnp.dot(x, wu[...], preferred_element_type=jnp.float32)
        act = (gate_pre * jax.nn.sigmoid(gate_pre) * up_pre).astype(jnp.bfloat16)
        y_scr[...] = lax.dot_general(act, wd[...], (((1,), (1,)), ((), ())), preferred_element_type=jnp.float32)

        def add_eight(b, _):
            base = pl.multiple_of(b * 8, 8)
            part = y_scr[pl.ds(base, 8), :]
            tokens = [token_ref[start + base + r] for r in range(8)]
            sums = [out_ref[pl.ds(tokens[r], 1), :] + part[r:r + 1, :] * gate_ref[start + base + r] for r in range(8)]
            for r in range(8):
                out_ref[pl.ds(tokens[r], 1), :] = sums[r]
            return 0

        def add_one(r, _):
            token = token_ref[start + r]
            out_ref[pl.ds(token, 1), :] = out_ref[pl.ds(token, 1), :] + y_scr[pl.ds(r, 1), :] * gate_ref[start + r]
            return 0

        full = lax.div(count, 8)
        lax.fori_loop(0, full, add_eight, 0)
        lax.fori_loop(full * 8, count, add_one, 0)


def run_experts(h_rows, tables, place, tokens, gates, gate_parts, up_parts, down_parts):
    tile_expert, tile_start, tile_count, num_tiles = tables
    place = jnp.stack([place, num_tiles])
    rows, hidden = h_rows.shape
    _, depth, width = gate_parts[0].shape
    whole = lambda i, *_: (0, 0)
    pick = lambda i, te, *_: (te[i], 0, 0)
    grid_spec = pltpu.PrefetchScalarGridSpec(
        num_scalar_prefetch=6,
        grid=(tile_expert.shape[0],),
        in_specs=[pl.BlockSpec((rows, hidden), whole, pipeline_mode=pl.Buffered(1))]
        + [pl.BlockSpec((1, depth, width), pick)] * 12,
        out_specs=pl.BlockSpec((rows, hidden), whole, pipeline_mode=pl.Buffered(1)),
        scratch_shapes=[
            pltpu.VMEM((ROW_TILE, hidden), jnp.float32),
            pltpu.VMEM((ROW_TILE, hidden), jnp.float32),
            pltpu.VMEM((hidden, width), jnp.bfloat16),
            pltpu.VMEM((hidden, width), jnp.bfloat16),
            pltpu.VMEM((hidden, width), jnp.bfloat16),
        ],
    )
    return pl.pallas_call(
        moe_kernel,
        grid_spec=grid_spec,
        out_shape=jax.ShapeDtypeStruct((rows, hidden), jnp.float32),
        compiler_params=pltpu.CompilerParams(vmem_limit_bytes=VMEM_LIMIT),
        name="experts",
    )(tile_expert, tile_start, tile_count, place, tokens, gates, h_rows, *gate_parts, *up_parts, *down_parts)


def tile_tables(sizes, first_expert, experts, max_pairs):
    order = jnp.arange(sizes.shape[0], dtype=jnp.int32)
    offsets = jnp.sum(jnp.where(order[None, :] < order[:, None], sizes[None, :], 0), axis=1)
    count = lax.dynamic_slice_in_dim(sizes, first_expert, experts)
    offset = lax.dynamic_slice_in_dim(offsets, first_expert, experts)
    tiles = (count + ROW_TILE - 1) // ROW_TILE
    local = jnp.arange(experts, dtype=jnp.int32)
    first_tile = jnp.sum(jnp.where(local[None, :] < local[:, None], tiles[None, :], 0), axis=1)
    num_tiles = jnp.sum(tiles)
    last = jnp.max(jnp.where(tiles > 0, local, 0))
    max_tiles = (max_pairs - experts) // ROW_TILE + experts
    tile = jnp.arange(max_tiles, dtype=jnp.int32)
    mine = (tile[:, None] >= first_tile[None, :]) & (tile[:, None] < (first_tile + tiles)[None, :])
    pick = lambda values: jnp.sum(jnp.where(mine, values, 0), axis=1).astype(jnp.int32)
    done = (tile[:, None] - first_tile[None, :]) * ROW_TILE
    return jnp.where(tile < num_tiles, pick(local[None, :]), last), pick(offset[None, :] + done), pick(jnp.minimum(count[None, :] - done, ROW_TILE)), num_tiles.astype(jnp.int32)


def solution(mesh):
    token_spec = P(('rep', 'tok', 'mp'))
    row_spec = P(('rep', 'tok', 'mp'), None)
    head_weight = P(None, 'tok', 'mp', None)
    in_specs = (row_spec, token_spec, row_spec, row_spec, head_weight, head_weight, head_weight, P(None, 'mp', None, 'tok'), P(None, None, 'tok', 'mp'), P(None, None, 'tok', 'mp'), P(None, None, 'mp', 'tok'), P(None, None), P(None, None))

    def swap_mp(value):
        return lax.ppermute(value, 'mp', [(0, 1), (1, 0)])

    def swap_chip(value):
        return lax.ppermute(value, 'tok', [(i, i ^ 2) for i in range(4)])

    def swap_core(value):
        return lax.ppermute(value, 'tok', [(i, i ^ 1) for i in range(4)])

    def layers(hidden_in, seg_ids, expert_ids, expert_gates, w_query, w_key, w_value, w_out, w_gate, w_up, w_down, gain_attn, gain_mlp):
        num_layers, depth, q_local, head_dim = w_query.shape
        num_experts = w_gate.shape[1]
        rows, hidden = hidden_in.shape
        half_experts = num_experts // 2
        chunk = half_experts // CHUNKS
        m = lax.axis_index('mp')
        t = lax.axis_index('tok')
        chip = t // 2
        place = t.astype(jnp.int32)

        def join(mine, other, axis=0):
            first = jnp.where(m == 0, mine, other)
            second = jnp.where(m == 0, other, mine)
            return jnp.concatenate([first, second], axis=axis)

        def gather_mp(value):
            return join(value, swap_mp(value))

        qkv_local = jnp.concatenate([w.reshape(num_layers, depth, q_local * head_dim) for w in (w_query, w_key, w_value)], axis=2)
        qkv_all = lax.all_gather(qkv_local, 'tok', axis=1, tiled=True)
        out_all = lax.all_gather(w_out.reshape(num_layers, q_local * head_dim, depth), ('mp', 'tok'), axis=0)
        out_all = out_all.reshape(2, 4, num_layers, q_local * head_dim, depth).transpose(2, 0, 3, 1, 4).reshape(num_layers, 2 * q_local * head_dim, hidden)

        def rotated(weight):
            parts = weight.reshape(hidden, q_local, 2, head_dim // 2)
            return jnp.concatenate([-parts[:, :, 1:], parts[:, :, :1]], axis=2).reshape(hidden, q_local * head_dim)

        seg_full = gather_mp(seg_ids)
        starts = request_starts(seg_full)
        seq_len = seg_full.shape[0]
        positions = jnp.arange(seq_len, dtype=jnp.int32) - starts
        inv_freq = jnp.power(ROPE_BASE, -jnp.arange(head_dim // 2, dtype=jnp.float32) * 2.0 / head_dim)
        angles = positions.astype(jnp.float32)[:, None] * inv_freq
        cosines = jnp.tile(jnp.cos(angles), (1, 4))
        sines = jnp.tile(jnp.sin(angles), (1, 4))

        flat_ids = gather_mp(expert_ids).reshape(2 * seq_len)
        flat_gates = gather_mp(expert_gates).reshape(2 * seq_len)
        pair_token = jnp.arange(2 * seq_len, dtype=jnp.int32) // 2
        _, tokens_own, gates_own = lax.sort((flat_ids, pair_token, flat_gates), num_keys=1)
        sizes_own = jnp.sum((flat_ids[:, None] == jnp.arange(num_experts, dtype=jnp.int32)[None, :]).astype(jnp.int32), axis=0)
        pad = jnp.zeros((8,), jnp.int32)
        ints_own = jnp.concatenate([sizes_own, tokens_own, pad])
        floats_own = jnp.concatenate([gates_own, pad.astype(jnp.float32)])
        ints_far = swap_chip(ints_own)
        floats_far = swap_chip(floats_own)
        routing = []
        for ints, floats in ((ints_far, floats_far), (ints_own, floats_own)):
            tables = [tile_tables(ints[:num_experts], chip * half_experts + c * chunk, chunk, 2 * seq_len) for c in range(CHUNKS)]
            routing.append((tables, ints[num_experts:], floats))

        weights = (w_gate, w_up, jnp.swapaxes(w_down, 2, 3))

        def launch(units, gate):
            held = weights if gate is None else lax.optimization_barrier((weights, gate))[0]
            for layer, c, kind in units:
                weight = held[kind]
                piece = lambda base: lax.dynamic_slice(weight, (layer, base * half_experts + c * chunk, 0, 0), (1, chunk) + weight.shape[2:])[0]
                far = lax.optimization_barrier(piece(1 - chip))
                near = lax.optimization_barrier(piece(chip))
                crossed = swap_chip(far)
                bulk[layer, c, kind] = near, crossed

        def spread(near, crossed):
            return near, swap_core(near), crossed, swap_core(crossed)

        half = rows // 2
        bulk = {}

        launch([(0, 0, 0), (0, 0, 1), (0, 0, 2)], None)
        residual = hidden_in.astype(jnp.float32)
        for layer in range(num_layers):
            q_w, k_w, v_w = jnp.split(qkv_all[layer], 3, axis=1)
            weight = jnp.concatenate([q_w, rotated(q_w), k_w, rotated(k_w), v_w], axis=1)
            normed = gather_mp(rms_norm(residual, gain_attn[layer]))
            q, k, v = project_qkv(normed, weight, cosines, sines)
            attn = attention(q, k, v, starts)
            keep = lax.dynamic_slice_in_dim(attn, m * rows, rows, 0)
            send = lax.dynamic_slice_in_dim(attn, (1 - m) * rows, rows, 0)
            attn_full = join(keep, swap_mp(send), axis=1)
            residual = residual + jnp.dot(attn_full, out_all[layer], preferred_element_type=jnp.float32)
            normed = rms_norm(residual, gain_mlp[layer])
            far_half = swap_chip(normed)
            if layer == 0:
                launch([(0, 1, 0), (0, 1, 1), (0, 1, 2), (1, 0, 0)], normed)
            else:
                launch([(1, 1, 1), (1, 1, 2)], normed)
            h_own = gather_mp(normed).astype(jnp.float32)
            h_far = gather_mp(far_half).astype(jnp.float32)
            parts = [None, None]
            for c in range(CHUNKS):
                gate_parts, up_parts, down_parts = [spread(*bulk[layer, c, kind]) for kind in range(3)]
                for s, h_rows in enumerate((h_far, h_own)):
                    tables, tokens, gates = routing[s]
                    got = run_experts(h_rows, tables[c], place, tokens, gates, gate_parts, up_parts, down_parts)
                    parts[s] = got if parts[s] is None else parts[s] + got
            far_sum, own_sum = parts
            pick = lambda value, which, part: lax.dynamic_slice_in_dim(value, which * rows + part * half, half, 0)
            far_other_1, far_mine_1, far_other_0, far_mine_0 = lax.optimization_barrier(tuple(pick(far_sum, which, part) for which, part in ((1 - m, 1), (m, 1), (1 - m, 0), (m, 0))))
            via_chip = swap_chip(far_other_1)
            mine_1 = swap_chip(far_mine_1)
            via_mp = swap_mp(far_other_0)
            if layer == 0:
                launch([(1, 0, 1), (1, 0, 2), (1, 1, 0)], via_mp)
            sent_0 = lax.optimization_barrier(far_mine_0 + via_mp)
            mine_0 = swap_chip(sent_0)
            own_other_0, own_other_1, own_0, own_1 = lax.optimization_barrier(tuple(pick(own_sum, which, part) for which, part in ((1 - m, 0), (1 - m, 1), (m, 0), (m, 1))))
            other_0 = swap_mp(own_other_0)
            other_1 = swap_mp(own_other_1 + via_chip)
            top = own_0 + other_0 + mine_0
            bottom = own_1 + other_1 + mine_1
            residual = residual + jnp.concatenate([top, bottom], axis=0)
        return residual

    return jax.shard_map(layers, mesh=mesh, in_specs=in_specs, out_specs=row_spec, check_vma=False)
```
